128 devices in a mesh: grid: 8 (over x, z_lo), band: 16 (over z_hi, y, core).
Axes of the slice: x: 4, y: 4, z: 4 (z_hi: 2, z_lo: 2; z = z_hi * 2 + z_lo), core: 2. Of those that a mesh axis runs over, the one named last changes fastest.
Arguments:
- orbitals: float32 [320, 32, 64, 128], P('band', 'grid'), may hold values from -6 to 6
- occupation: float32 [320], P('band'), may hold values from 0.003125 to 0.025
- core_density: float32 [32, 64, 128], P('grid'), may hold values from 0.2 to 2
- local_potential: float32 [32, 64, 128], P('grid'), may hold values from -6 to 6
Outputs:
- applied: float32 [320, 32, 64, 128], P('band', 'grid')
The draws below stay inside these ranges and needn't reach their ends.
All inputs are finite; a program needn't handle non-finite values.
Results may differ from the reference program's by a relative error of at most 0.0001.
Values sent between devices are 32-bit elements; how exact they have to be, the bound alone decides.
No kernel may reach another device: no remote copies, remote signals or barrier semaphores. Data moves between devices by JAX's collectives and lax.ppermute only.
A program may use at most 192 MiB of HBM per device.

```python
import math
import jax
import jax.numpy as jnp
from jax import lax

NY = 64
NZ = 128
BANDS = 320
NX = 32


def block_levels(key, shape, shards, low, high):
    loudness = 1.0
    for dim, parts in shards:
        draws = jax.random.uniform(jax.random.fold_in(jax.random.fold_in(key, 6), dim), (parts,), jnp.float32, low / len(shards), high / len(shards))
        loudness = loudness * jnp.repeat(jnp.exp(draws), shape[dim] // parts).reshape((-1,) + (1,) * (len(shape) - 1 - dim))
    return loudness


def normal_values(own_key, dims, scale, most, split=(), kind=jnp.bfloat16):
    drawn = jax.random.normal(own_key, dims, jnp.float32) * scale
    if len(split) > 0:
        drawn = block_levels(own_key, dims, split, -0.22, 0.18) * drawn
    return jnp.clip(drawn, min=-most, max=most).astype(kind)


def setup_inputs(seed: int = 0) -> dict:
    key_of = jax.random.split(jax.random.key(seed), 5)
    return {
        "orbitals": normal_values(key_of[0], (BANDS, NX, NY, NZ), 1.0, 6.0, ((0, 16), (1, 8)), jnp.float32),
        "occupation": jnp.clip(jnp.exp(math.log(0.025) - 2.0794415 * jax.random.uniform(key_of[1], (BANDS,), jnp.float32) ** block_levels(key_of[1], (BANDS,), ((0, 16),), -0.2, 0.2)), 0.003125, 0.025),
        "core_density": jnp.clip(jnp.exp(math.log(2.0) - 2.3025851 * jax.random.uniform(key_of[2], (NX, NY, NZ), jnp.float32) ** block_levels(key_of[2], (NX, NY, NZ), ((0, 8),), -0.2, 0.2)), 0.2, 2.0),
        "local_potential": normal_values(key_of[3], (NX, NY, NZ), 1.0, 6.0, ((0, 8),), jnp.float32),
    }


def derive(field, axis):
    ahead = jnp.roll(field, -1, axis) - jnp.roll(field, 1, axis)
    far = jnp.roll(field, -2, axis) - jnp.roll(field, 2, axis)
    return (8.0 * ahead - far) / 12.0


def pointwise(density, kinetic, local_potential):
    uniform = 2.871 * jnp.power(density, 5.0 / 3.0)
    ratio = kinetic / (kinetic + uniform)
    potential = local_potential - 0.7386 * jnp.power(density, 1.0 / 3.0) * (1.0 + 0.3 * ratio)
    weight = 1.0 + 0.4 * ratio
    return potential, weight


def reference(orbitals, occupation, core_density, local_potential):
    blocks = orbitals.reshape((BANDS // 8, 8) + orbitals.shape[1:])
    weights = occupation.reshape((BANDS // 8, 8))

    def accumulate(carry, item):
        block, occ = item
        occ4 = occ[:, None, None, None]
        squares = derive(block, 1) ** 2 + derive(block, 2) ** 2 + derive(block, 3) ** 2
        rho = carry[0] + jnp.sum(occ4 * block * block, axis=0)
        tau = carry[1] + 0.5 * jnp.sum(occ4 * squares, axis=0)
        return (rho, tau), None

    start = (jnp.zeros(core_density.shape, jnp.float32), jnp.zeros(core_density.shape, jnp.float32))
    (rho_sum, tau_sum), _ = lax.scan(accumulate, start, (blocks, weights))
    potential, weight = pointwise(core_density + rho_sum, tau_sum, local_potential)

    def apply_block(block):
        result = -0.5 * (derive(weight[None] * derive(block, 1), 1) + derive(weight[None] * derive(block, 2), 2) + derive(weight[None] * derive(block, 3), 3))
        return result + potential[None] * block

    applied = lax.map(apply_block, blocks)
    return applied.reshape(orbitals.shape)
```

```python
import jax
import jax.numpy as jnp
from jax import lax
from jax.experimental import pallas as pl
from jax.experimental.pallas import tpu as pltpu
from jax.sharding import PartitionSpec as P


F32 = jnp.float32
SLABS = 8
GROUP = 16
ROWS = 32

PAIR = [(i, i ^ 1) for i in range(SLABS)]
OUTWARD = [(i, (i - 2) % SLABS if i % 2 == 0 else (i + 2) % SLABS) for i in range(SLABS)]
INWARD = [(i, (i + 2) % SLABS if i % 2 == 0 else (i - 2) % SLABS) for i in range(SLABS)]
ACROSS = [
    (g * GROUP + b, (g ^ 1) * GROUP + (b ^ 8)) for g in range(SLABS) for b in range(GROUP)
]


def partners(bits):
    return [(i, i ^ bits) for i in range(GROUP)]


def place():
    lower = lax.axis_index("grid") % 2
    band = lax.axis_index("band")
    half = lower ^ (band // 8)
    return lower, half, band % 2, band


def mirrored(index, lower, count):
    return jnp.where(lower == 1, count - 1 - index, index)


def rows_of(half):
    return pl.ds(pl.multiple_of(half * ROWS, ROWS), ROWS)


def stencil(x, axis):
    count = x.shape[axis]
    ahead = pltpu.roll(x, count - 2, axis) - x
    near = pltpu.roll(ahead, 1, axis)
    far = ahead + pltpu.roll(ahead, 2, axis)
    return 8.0 * near - far


def spread(before2, before1, after1, after2):
    return 8.0 * (after1 - before1) - (after2 - before2)


def call(kernel, outs, *args, **kwargs):
    return pl.pallas_call(
        kernel, out_shape=[jax.ShapeDtypeStruct(s, F32) for s in outs], **kwargs
    )(*args)


def pack(orbitals, first):
    bands = orbitals.shape[0]
    step = 4

    def kernel(u_ref, other_ref, own_ref):
        lower, half, _, _ = place()
        for k in range(2):
            layer = mirrored(first + k, lower, 4)
            other_ref[:, k] = u_ref[:, layer, rows_of(1 - half), :]
            own_ref[:, k] = u_ref[:, layer, rows_of(half), :]

    block = pl.BlockSpec((step, 2, ROWS, 128), lambda i: (i, 0, 0, 0))
    return call(
        kernel,
        [(bands, 2, ROWS, 128)] * 2,
        orbitals,
        grid=(bands // step,),
        in_specs=[pl.BlockSpec((step, 4, 64, 128), lambda i: (i, 0, 0, 0))],
        out_specs=[block, block],
    )


def statistics(orbitals, occupation, core_density):
    bands = orbitals.shape[0]

    def kernel(occ_ref, u_ref, core_ref, own_ref, other_ref, rho_ref, tau_ref):
        lower, half, _, band = place()
        slot = mirrored(pl.program_id(0), lower, 4)

        def one(b, sums):
            rho, tau = sums
            x = u_ref[b, 0]
            weight = occ_ref[b]
            along_y = stencil(x, 0)
            along_z = stencil(x, 1)
            return (
                rho + weight * (x * x),
                tau + weight * (along_y * along_y + along_z * along_z),
            )

        zero = jnp.zeros((64, 128), F32)
        rho, tau = lax.fori_loop(0, bands, one, (zero, zero))
        rho_ref[...] = rho + jnp.where(band == 0, core_ref[0], zero)
        tau_ref[...] = tau * (0.5 / 144.0)
        own_ref[0, slot] = rho_ref[rows_of(half), :]
        own_ref[1, slot] = tau_ref[rows_of(half), :]
        other_ref[0, slot] = rho_ref[rows_of(1 - half), :]
        other_ref[1, slot] = tau_ref[rows_of(1 - half), :]

    whole = pl.BlockSpec((2, 4, ROWS, 128), lambda i: (0, 0, 0, 0))
    return call(
        kernel,
        [(2, 4, ROWS, 128)] * 2,
        occupation,
        orbitals,
        core_density,
        grid=(4,),
        in_specs=[
            pl.BlockSpec(memory_space=pltpu.SMEM),
            pl.BlockSpec((bands, 1, 64, 128), lambda i: (0, i, 0, 0)),
            pl.BlockSpec((1, 64, 128), lambda i: (i, 0, 0)),
        ],
        out_specs=[whole, whole],
        scratch_shapes=[pltpu.VMEM((64, 128), F32)] * 2,
    )


def kinetic_x(occupation, outer, inner, far_outer, far_inner, after, before, sums_own, sums_far):
    bands = outer.shape[0]

    def kernel(
        occ_ref, outer_ref, inner_ref, far_outer_ref, far_inner_ref, after_ref, before_ref,
        own_ref, far_ref, keep_ref, send_ref, all_ref,
    ):
        lower, _, core, _ = place()
        for t in range(ROWS // 8):
            r = pl.ds(8 * t, 8)

            def one(b, sums):
                v = (
                    before_ref[b, 1, r], before_ref[b, 0, r],
                    outer_ref[b, 0, r], outer_ref[b, 1, r],
                    inner_ref[b, 0, r], inner_ref[b, 1, r],
                    far_inner_ref[b, 1, r], far_inner_ref[b, 0, r],
                    far_outer_ref[b, 1, r], far_outer_ref[b, 0, r],
                    after_ref[b, 0, r], after_ref[b, 1, r],
                )
                weight = occ_ref[b]
                out = []
                for s in range(8):
                    g = spread(v[s], v[s + 1], v[s + 3], v[s + 4])
                    out.append(sums[s] + weight * (g * g))
                return tuple(out)

            sums = lax.fori_loop(0, bands, one, (jnp.zeros((8, 128), F32),) * 8)
            for s in range(8):
                ref, k = (own_ref, s) if s < 4 else (far_ref, 7 - s)
                all_ref[0, s, r] = ref[0, k, r]
                all_ref[1, s, r] = ref[1, k, r] + sums[s] * (0.5 / 144.0)
        for j in range(4):
            keep_ref[:, j] = all_ref[:, mirrored(4 * core + j, lower, 8)]
            send_ref[:, j] = all_ref[:, mirrored(4 * (1 - core) + j, lower, 8)]

    vmem = pl.BlockSpec(memory_space=pltpu.VMEM)
    return call(
        kernel,
        [(2, 4, ROWS, 128)] * 2,
        occupation, outer, inner, far_outer, far_inner, after, before, sums_own, sums_far,
        in_specs=[pl.BlockSpec(memory_space=pltpu.SMEM)] + [vmem] * 8,
        out_specs=[vmem, vmem],
        scratch_shapes=[pltpu.VMEM((2, 8, ROWS, 128), F32)],
    )


def pointwise(sums):
    density, kinetic = sums[0], sums[1]
    root = jnp.power(density, 1.0 / 3.0)
    ratio = kinetic / (kinetic + 2.871 * (density * (root * root)))
    return jnp.stack([1.0 + 0.4 * ratio, -0.7386 * root * (1.0 + 0.3 * ratio)])


def assemble(mine, theirs, local_potential):
    def kernel(mine_ref, theirs_ref, local_ref, weight_ref, potential_ref, edge_ref, all_ref):
        lower, half, core, _ = place()
        for side in range(2):
            r = rows_of(half if side == 0 else 1 - half)
            for j in range(4):
                all_ref[:, 4 * core + j, r, :] = mine_ref[side, :, j]
                all_ref[:, 4 * (1 - core) + j, r, :] = theirs_ref[side, :, j]
        for s in range(8):
            weight_ref[s] = all_ref[0, mirrored(s, lower, 8)]
        for k in range(4):
            potential_ref[k] = local_ref[k] + all_ref[1, 4 * lower + k]
        edge_ref[0] = weight_ref[7]
        edge_ref[1] = weight_ref[6]

    vmem = pl.BlockSpec(memory_space=pltpu.VMEM)
    return call(
        kernel,
        [(8, 64, 128), (4, 64, 128), (2, 64, 128)],
        mine, theirs, local_potential,
        in_specs=[vmem] * 3,
        out_specs=[vmem] * 3,
        scratch_shapes=[pltpu.VMEM((2, 8, 64, 128), F32)],
    )


def in_plane(orbitals, weight, potential):
    bands = orbitals.shape[0]

    def kernel(u_ref, weight_ref, potential_ref, out_ref):
        lower = lax.axis_index("grid") % 2
        w = weight_ref[mirrored(pl.program_id(0), lower, 4)]
        v = potential_ref[0]

        def one(b, carry):
            x = u_ref[b, 0]
            both = stencil(w * stencil(x, 0), 0) + stencil(w * stencil(x, 1), 1)
            out_ref[b, 0] = v * x - (0.5 / 144.0) * both
            return carry

        lax.fori_loop(0, bands, one, 0)

    block = pl.BlockSpec((bands, 1, 64, 128), lambda i: (0, i, 0, 0))
    return call(
        kernel,
        [orbitals.shape],
        orbitals, weight, potential,
        grid=(4,),
        in_specs=[
            block,
            pl.BlockSpec((8, 64, 128), lambda i: (0, 0, 0)),
            pl.BlockSpec((1, 64, 128), lambda i: (i, 0, 0)),
        ],
        out_specs=[block],
    )[0]


def add_x(partial, orbitals, halves, weight, edge):
    bands = orbitals.shape[0]
    step = 4

    def kernel(partial_ref, u_ref, *refs):
        chunk_refs, weight_ref, edge_ref, out_ref = refs[:8], refs[8], refs[9], refs[10]
        lower, half, _, _ = place()
        layers = [mirrored(s, lower, 4) for s in range(4)]
        for side in range(2):
            outer, inner, before, early = chunk_refs[4 * side : 4 * side + 4]
            for t in range(ROWS // 8):
                local = pl.ds(8 * t, 8)
                first = (half if side == 0 else 1 - half) * ROWS + 8 * t
                r = pl.ds(pl.multiple_of(first, 8), 8)
                w = [edge_ref[1, r], edge_ref[0, r]] + [weight_ref[s, r] for s in range(6)]

                def one(b, carry):
                    v = (
                        early[b, 1, local], early[b, 0, local],
                        before[b, 1, local], before[b, 0, local],
                        u_ref[b, layers[0], r], u_ref[b, layers[1], r],
                        u_ref[b, layers[2], r], u_ref[b, layers[3], r],
                        inner[b, 1, local], inner[b, 0, local],
                        outer[b, 1, local], outer[b, 0, local],
                    )
                    f = [w[k] * spread(v[k], v[k + 1], v[k + 3], v[k + 4]) for k in range(8)]
                    for s in range(4):
                        d = spread(f[s], f[s + 1], f[s + 3], f[s + 4])
                        out_ref[b, layers[s], r] = partial_ref[b, layers[s], r] - (0.5 / 144.0) * d
                    return carry

                lax.fori_loop(0, step, one, 0, unroll=True)

    block = pl.BlockSpec((step, 4, 64, 128), lambda i: (i, 0, 0, 0))
    chunk = pl.BlockSpec((step, 2, ROWS, 128), lambda i: (i, 0, 0, 0))
    return call(
        kernel,
        [orbitals.shape],
        partial, orbitals, *halves, weight, edge,
        grid=(bands // step,),
        in_specs=[block, block]
        + [chunk] * 8
        + [pl.BlockSpec((8, 64, 128), lambda i: (0, 0, 0)), pl.BlockSpec((2, 64, 128), lambda i: (0, 0, 0))],
        out_specs=[block],
    )[0]


def per_device(orbitals, occupation, core_density, local_potential):
    outer_other, outer_own = pack(orbitals, 0)
    inner_other, inner_own = pack(orbitals, 2)
    c1 = lax.ppermute(outer_other, "grid", PAIR)
    after = lax.ppermute(outer_own, "grid", OUTWARD)
    c2 = lax.ppermute(inner_other, "grid", PAIR)
    sums_own, sums_other = statistics(orbitals, occupation, core_density)
    sums_far = lax.ppermute(sums_other, "grid", PAIR)
    c3 = lax.ppermute(outer_own, "grid", PAIR)
    c4 = lax.ppermute(inner_own, "grid", PAIR)
    before1 = lax.ppermute(c1, "grid", INWARD)
    before2 = lax.ppermute(c2, "grid", INWARD)
    before3 = lax.ppermute(c3, "grid", INWARD)
    before4 = lax.ppermute(c4, "grid", INWARD)
    keep, send = kinetic_x(
        occupation, outer_own, inner_own, c1, c2, after, before1, sums_own, sums_far
    )
    sums = keep + lax.ppermute(send, "band", partners(1))
    sums = sums + lax.ppermute(sums, "band", partners(2))
    sums = sums + lax.ppermute(sums, "band", partners(6))
    sums = sums + lax.ppermute(sums, ("grid", "band"), ACROSS)
    fields = pointwise(sums)
    mine = jnp.stack([fields, lax.ppermute(fields, "grid", PAIR)])
    theirs = lax.ppermute(mine, "band", partners(1))
    weight, potential, edge = assemble(mine, theirs, local_potential)
    edge = lax.ppermute(edge, "grid", INWARD)
    partial = in_plane(orbitals, weight, potential)
    halves = (c1, c2, before1, before2, c3, c4, before3, before4)
    return add_x(partial, orbitals, halves, weight, edge)


def solution(mesh):
    spec = P("band", "grid", None, None)
    return jax.shard_map(
        per_device,
        mesh=mesh,
        in_specs=(spec, P("band"), P("grid", None, None), P("grid", None, None)),
        out_specs=spec,
        check_vma=False,
    )
```

```python
import jax
import jax.numpy as jnp
from jax import lax
from jax.experimental import pallas as pl
from jax.experimental.pallas import tpu as pltpu
from jax.sharding import PartitionSpec as P


F32 = jnp.float32
SLABS = 8
GROUP = 16
ROWS = 32

PAIR = [(i, i ^ 1) for i in range(SLABS)]
OUTWARD = [(i, (i - 2) % SLABS if i % 2 == 0 else (i + 2) % SLABS) for i in range(SLABS)]
INWARD = [(i, (i + 2) % SLABS if i % 2 == 0 else (i - 2) % SLABS) for i in range(SLABS)]
ACROSS = [
    (g * GROUP + b, (g ^ 1) * GROUP + (b ^ 8)) for g in range(SLABS) for b in range(GROUP)
]


def partners(bits):
    return [(i, i ^ bits) for i in range(GROUP)]


def place():
    lower = lax.axis_index("grid") % 2
    band = lax.axis_index("band")
    half = lower ^ (band // 8)
    return lower, half, band % 2, band


def mirrored(index, lower, count):
    return jnp.where(lower == 1, count - 1 - index, index)


def rows_of(half):
    return pl.ds(pl.multiple_of(half * ROWS, ROWS), ROWS)


def stencil(x, axis):
    count = x.shape[axis]
    ahead = pltpu.roll(x, count - 2, axis) - x
    near = pltpu.roll(ahead, 1, axis)
    far = ahead + pltpu.roll(ahead, 2, axis)
    return 8.0 * near - far


def spread(before2, before1, after1, after2):
    return 8.0 * (after1 - before1) - (after2 - before2)


VMEM = pl.BlockSpec(memory_space=pltpu.VMEM)
SMEM = pl.BlockSpec(memory_space=pltpu.SMEM)


def call(name, kernel, outs, args, in_specs, out_specs, scratch=(), flops=0, **kwargs):
    return pl.pallas_call(
        kernel,
        name=name,
        out_shape=[jax.ShapeDtypeStruct(s, F32) for s in outs],
        in_specs=in_specs,
        out_specs=out_specs,
        scratch_shapes=[pltpu.VMEM(s, F32) for s in scratch],
        compiler_params=pltpu.CompilerParams(vmem_limit_bytes=6 << 20),
        cost_estimate=pl.CostEstimate(flops=flops, bytes_accessed=0, transcendentals=0),
        **kwargs,
    )(*args)


def statistics(orbitals, occupation, core_density):
    bands = orbitals.shape[0]

    def kernel(occ_ref, u_ref, core_ref, own_ref, other_ref, grad_y_ref, grad_z_ref, rho_ref, tau_ref):
        lower, half, _, band = place()
        for layer in range(4):

            def one(b, sums):
                rho, tau = sums
                x = u_ref[b, layer]
                weight = occ_ref[b]
                along_y = stencil(x, 0)
                along_z = stencil(x, 1)
                grad_y_ref[b, layer] = along_y
                grad_z_ref[b, layer] = along_z
                return (
                    rho + weight * (x * x),
                    tau + weight * (along_y * along_y + along_z * along_z),
                )

            zero = jnp.zeros((64, 128), F32)
            rho, tau = lax.fori_loop(0, bands, one, (zero, zero), unroll=4)
            rho_ref[...] = rho + jnp.where(band == 0, core_ref[layer], zero)
            tau_ref[...] = tau * (0.5 / 144.0)
            for side, ref in ((half, own_ref), (1 - half, other_ref)):
                ref[0, layer] = rho_ref[rows_of(side), :]
                ref[1, layer] = tau_ref[rows_of(side), :]

    return call(
        "statistics",
        kernel,
        [(2, 4, ROWS, 128)] * 2 + [orbitals.shape] * 2,
        (occupation, orbitals, core_density),
        [SMEM, VMEM, VMEM],
        [VMEM] * 4,
        scratch=[(64, 128)] * 2,
        flops=1 << 30,
    )


def kinetic_x(occupation, chunks, sums_own, sums_far):
    before, outer, inner, far_inner, far_outer, after = chunks
    bands = outer.shape[0]

    def kernel(occ_ref, *refs):
        chunk_refs, (own_ref, far_ref, keep_ref, send_ref, all_ref) = refs[:6], refs[6:]
        lower, _, core, _ = place()
        order = (mirrored(0, lower, 2), mirrored(1, lower, 2))
        for t in range(ROWS // 8):
            r = pl.ds(8 * t, 8)

            def one(b, sums):
                v = [ref[b, k, r] for ref in chunk_refs for k in order]
                weight = occ_ref[b]
                out = []
                for s in range(8):
                    g = spread(v[s], v[s + 1], v[s + 3], v[s + 4])
                    out.append(sums[s] + weight * (g * g))
                return tuple(out)

            sums = lax.fori_loop(0, bands, one, (jnp.zeros((8, 128), F32),) * 8, unroll=2)
            for s in range(8):
                ref, k = (own_ref, mirrored(s, lower, 4)) if s < 4 else (far_ref, mirrored(s - 4, lower, 4))
                all_ref[0, s, r] = ref[0, k, r]
                all_ref[1, s, r] = ref[1, k, r] + sums[s] * (0.5 / 144.0)
        for j in range(4):
            keep_ref[:, j] = all_ref[:, mirrored(4 * core + j, lower, 8)]
            send_ref[:, j] = all_ref[:, mirrored(4 * (1 - core) + j, lower, 8)]

    return call(
        "kinetic_x",
        kernel,
        [(2, 4, ROWS, 128)] * 2,
        (occupation, *chunks, sums_own, sums_far),
        [SMEM] + [VMEM] * 8,
        [VMEM] * 2,
        scratch=[(2, 8, ROWS, 128)],
        flops=1 << 28,
    )


def pointwise(sums):
    density, kinetic = sums[0], sums[1]
    root = jnp.power(density, 1.0 / 3.0)
    ratio = kinetic / (kinetic + 2.871 * (density * (root * root)))
    return jnp.stack([1.0 + 0.4 * ratio, -0.7386 * root * (1.0 + 0.3 * ratio)])


def assemble(mine, theirs, local_potential):
    def kernel(mine_ref, theirs_ref, local_ref, weight_ref, potential_ref, edge_ref, all_ref):
        lower, half, core, _ = place()
        for side in range(2):
            r = rows_of(half if side == 0 else 1 - half)
            for j in range(4):
                all_ref[:, 4 * core + j, r, :] = mine_ref[side, :, j]
                all_ref[:, 4 * (1 - core) + j, r, :] = theirs_ref[side, :, j]
        for s in range(8):
            weight_ref[s] = all_ref[0, mirrored(s, lower, 8)]
        for k in range(4):
            potential_ref[k] = local_ref[k] + all_ref[1, 4 * lower + k]
        edge_ref[0] = weight_ref[7]
        edge_ref[1] = weight_ref[6]

    return call(
        "assemble",
        kernel,
        [(8, 64, 128), (4, 64, 128), (2, 64, 128)],
        (mine, theirs, local_potential),
        [VMEM] * 3,
        [VMEM] * 3,
        scratch=[(2, 8, 64, 128)],
        flops=1 << 27,
    )


def in_plane(orbitals, grad_y, grad_z, weight, potential):
    bands = orbitals.shape[0]

    def kernel(u_ref, grad_y_ref, grad_z_ref, weight_ref, potential_ref, out_ref):
        lower = lax.axis_index("grid") % 2
        for layer in range(4):
            w = weight_ref[mirrored(layer, lower, 4)] * (0.5 / 144.0)
            v = potential_ref[layer]

            def one(b, carry):
                both = stencil(w * grad_y_ref[b, layer], 0) + stencil(w * grad_z_ref[b, layer], 1)
                out_ref[b, layer] = v * u_ref[b, layer] - both
                return carry

            lax.fori_loop(0, bands, one, 0, unroll=4)

    return call(
        "in_plane",
        kernel,
        [orbitals.shape],
        (orbitals, grad_y, grad_z, weight, potential),
        [VMEM] * 5,
        [VMEM],
        flops=1 << 30,
    )[0]


def add_x(partial, orbitals, halves, weight, edge):
    bands = orbitals.shape[0]
    step = 4

    def kernel(partial_ref, u_ref, *refs):
        chunk_refs, weight_ref, edge_ref, out_ref = refs[:8], refs[8], refs[9], refs[10]
        lower, half, _, _ = place()
        layers = [mirrored(s, lower, 4) for s in range(4)]
        order = (mirrored(0, lower, 2), mirrored(1, lower, 2))
        start = pl.program_id(0) * step
        for side in range(2):
            early, before, inner, outer = chunk_refs[4 * side : 4 * side + 4]
            for t in range(ROWS // 8):
                local = pl.ds(8 * t, 8)
                first = (half if side == 0 else 1 - half) * ROWS + 8 * t
                r = pl.ds(pl.multiple_of(first, 8), 8)
                w = [edge_ref[1, r], edge_ref[0, r]] + [weight_ref[s, r] for s in range(6)]
                w = [x * (0.5 / 144.0) for x in w]

                def one(k, carry):
                    b = start + k
                    v = (
                        [early[b, i, local] for i in order]
                        + [before[b, i, local] for i in order]
                        + [u_ref[b, i, r] for i in layers]
                        + [inner[b, i, local] for i in order]
                        + [outer[b, i, local] for i in order]
                    )
                    f = [w[j] * spread(v[j], v[j + 1], v[j + 3], v[j + 4]) for j in range(8)]
                    for s in range(4):
                        d = spread(f[s], f[s + 1], f[s + 3], f[s + 4])
                        out_ref[k, layers[s], r] = partial_ref[b, layers[s], r] - d
                    return carry

                lax.fori_loop(0, step, one, 0, unroll=2)

    return call(
        "add_x",
        kernel,
        [orbitals.shape],
        (partial, orbitals, *halves, weight, edge),
        [VMEM] * 12,
        [pl.BlockSpec((step, 4, 64, 128), lambda i: (i, 0, 0, 0))],
        grid=(bands // step,),
        flops=1 << 28,
    )[0]


def cut(orbitals):
    lower, half, _, _ = place()
    bands = orbitals.shape[0]

    def part(layer, side):
        return lax.dynamic_slice(orbitals, (0, layer, side * ROWS, 0), (bands, 2, ROWS, 128))

    outer, inner = 2 * lower, 2 - 2 * lower
    return part(outer, 1 - half), part(outer, half), part(inner, 1 - half), part(inner, half)


def per_device(orbitals, occupation, core_density, local_potential):
    outer_other, outer_own, inner_other, inner_own = cut(orbitals)
    c1 = lax.ppermute(outer_other, "grid", PAIR)
    after = lax.ppermute(outer_own, "grid", OUTWARD)
    c2 = lax.ppermute(inner_other, "grid", PAIR)
    sums_own, sums_other, grad_y, grad_z = statistics(orbitals, occupation, core_density)
    sums_far = lax.ppermute(sums_other, "grid", PAIR)
    c3 = lax.ppermute(outer_own, "grid", PAIR)
    c4 = lax.ppermute(inner_own, "grid", PAIR)
    before1 = lax.ppermute(c1, "grid", INWARD)
    before2 = lax.ppermute(c2, "grid", INWARD)
    before3 = lax.ppermute(c3, "grid", INWARD)
    before4 = lax.ppermute(c4, "grid", INWARD)
    keep, send = kinetic_x(
        occupation, (before1, outer_own, inner_own, c2, c1, after), sums_own, sums_far
    )
    sums = keep + lax.ppermute(send, "band", partners(1))
    sums = sums + lax.ppermute(sums, "band", partners(2))
    sums = sums + lax.ppermute(sums, "band", partners(6))
    sums = sums + lax.ppermute(sums, ("grid", "band"), ACROSS)
    fields = pointwise(sums)
    mine = jnp.stack([fields, lax.ppermute(fields, "grid", PAIR)])
    theirs = lax.ppermute(mine, "band", partners(1))
    weight, potential, edge = assemble(mine, theirs, local_potential)
    edge = lax.ppermute(edge, "grid", INWARD)
    partial = in_plane(orbitals, grad_y, grad_z, weight, potential)
    halves = (before2, before1, c2, c1, before4, before3, c4, c3)
    return add_x(partial, orbitals, halves, weight, edge)


def solution(mesh):
    spec = P("band", "grid", None, None)
    return jax.shard_map(
        per_device,
        mesh=mesh,
        in_specs=(spec, P("band"), P("grid", None, None), P("grid", None, None)),
        out_specs=spec,
        check_vma=False,
    )
```
